32 devices in a mesh: patch: 16 (over z, y, x), batch: 2 (over core).
Axes of the slice: x: 2, y: 2, z: 4, core: 2. Of those that a mesh axis runs over, the one named last changes fastest.
Arguments:
- tokens: bfloat16 [4096, 1152], P(('batch', 'patch')), parts along dimension 0, may hold values from -6 to 6
- slots: int32 [4096], P(('batch', 'patch')), parts along dimension 0, may hold values from 0 to 127, as said below
- counts: int32 [32], P(('batch', 'patch')), parts along dimension 0, may hold values from 32 to 128, as said below
- shift: float32 [1152], replicated, may hold values from -3 to 3
- scale: float32 [1152], replicated, may hold values from -3 to 3
- gate: float32 [1152], replicated, may hold values from -4 to 4
- w_qkv: bfloat16 [1152, 3456], replicated, may hold values from -1 to 1
- w_out: bfloat16 [1152, 1152], replicated, may hold values from -0.1875 to 0.1875
Outputs:
- result: bfloat16 [4096, 1152], P(('batch', 'patch')), parts along dimension 0
The draws below stay inside these ranges and needn't reach their ends.
There are 2 independent parts, one for each index of `batch`. The reference program is written for one: setup_inputs(seed, part) draws one part's arguments, and reference() takes and returns one part's arrays. A program takes and returns all parts, laid end to end along the dimension named above; an argument that names none is the same for every part. Nothing has to cross between parts.
Inputs may be any that keep to these rules, and one draw needn't show every extreme that they name: `counts`: at least a quarter of each block's slots are live. The live slots of all blocks of an image number exactly 80 times the number of patch devices, and all blocks of some device are full. `slots`: every token's slot is below its block's count, and every slot below the count holds at least one token.
All inputs are finite; a program needn't handle non-finite values.
Results may differ from the reference program's by a relative error of at most 0.011.
Values may be sent and summed in bfloat16 or wider, within the bound.
A program may use at most 192 MiB of HBM per device.

```python
import jax
import jax.numpy as jnp
from jax import lax

D = 1152
HEADS = 16
HD = 72
BLK = 128
BLK_DEV = 1
TOKENS = 2048


def merge_plan(key):
    block_total = TOKENS // BLK
    device_total = block_total // BLK_DEV
    extra = BLK - BLK // 4
    needed = 5 * TOKENS // 8 - block_total * (BLK // 4)
    base = jax.random.fold_in(key, 11)
    key_level, key_full, key_noise, key_perm, key_rest = jax.random.split(base, 5)
    level = jax.random.randint(key_level, (block_total,), 0, 4096).astype(jnp.int32)
    chosen = jax.random.randint(key_full, (), 0, device_total).astype(jnp.int32)
    owner = jnp.arange(block_total, dtype=jnp.int32) // BLK_DEV
    level = jnp.where(owner == chosen, 8192, level).astype(jnp.int32)
    noise = jax.random.randint(key_noise, (block_total, extra), 0, 4096).astype(jnp.int32)
    ranked = ((level[:, None] + noise) * (block_total * extra)).reshape(block_total * extra) + jnp.arange(block_total * extra, dtype=jnp.int32)
    ordered = jnp.sort(ranked)
    cutoff = ordered[block_total * extra - needed]
    picked = (ranked >= cutoff).astype(jnp.int32).reshape(block_total, extra)
    counts = (BLK // 4 + jnp.sum(picked, axis=1)).astype(jnp.int32)
    ranks = jax.vmap(lambda k: jax.random.permutation(k, BLK))(jax.random.split(key_perm, block_total)).astype(jnp.int32)
    spare = jax.random.randint(key_rest, (block_total, BLK), 0, BLK * BLK).astype(jnp.int32) % counts[:, None]
    slots = jnp.where(ranks < counts[:, None], ranks, spare).astype(jnp.int32)
    return (slots.reshape(TOKENS), counts)


def draw_slots(key, part):
    return merge_plan(key)[0]


def draw_counts(key, part):
    return merge_plan(key)[1]


def draw_tokens(key, part):
    key_base = jax.random.fold_in(jax.random.fold_in(key, 23), 0)
    drawn = jnp.clip(jax.random.normal(key_base, (TOKENS, D), jnp.float32), -6.0, 6.0)
    return drawn.astype(jnp.bfloat16)


def draw_w_qkv(key, part):
    key_base = jax.random.fold_in(jax.random.fold_in(key, 37), 0)
    base = jnp.clip(jax.random.normal(key_base, (D, 3 * D), jnp.float32), -6.0, 6.0) * D ** (-0.5)
    return jnp.clip(base, -1.0, 1.0).astype(jnp.bfloat16)


def gaussian(own_key, extent, deviation, limit, kind=jnp.bfloat16):
    drawn = jax.random.normal(own_key, extent, jnp.float32) * deviation
    return jnp.minimum(jnp.maximum(drawn, -limit), limit).astype(kind)


def setup_inputs(seed: int = 0, part: int = 0) -> dict:
    key_of = jax.random.split(jax.random.key(seed), 9)
    part_splits = jax.random.split(jax.random.fold_in(key_of[8], part), 9)
    tokens = draw_tokens(jax.random.fold_in(jax.random.fold_in(key_of[8], part), 71), part)
    slots = draw_slots(jax.random.fold_in(jax.random.fold_in(key_of[8], part), 71), part)
    counts = draw_counts(jax.random.fold_in(jax.random.fold_in(key_of[8], part), 71), part)
    shift = gaussian(key_of[3], (D,), 0.5, 3.0, jnp.float32)
    scale = gaussian(key_of[4], (D,), 0.5, 3.0, jnp.float32)
    gate = gaussian(key_of[5], (D,), 1.0, 4.0, jnp.float32)
    w_qkv = draw_w_qkv(jax.random.fold_in(key_of[8], 71), part)
    w_out = gaussian(key_of[7], (D, D), D ** -0.5, 0.1875)
    return dict(tokens=tokens, slots=slots, counts=counts, shift=shift, scale=scale, gate=gate, w_qkv=w_qkv, w_out=w_out)


def layer_norm(merged, shift, scale):
    values = merged.astype(jnp.float32)
    center = lax.optimization_barrier(jnp.mean(values, axis=-1, keepdims=True))
    spread = lax.optimization_barrier(jnp.mean((values - center) ** 2, axis=-1, keepdims=True))
    return ((values - center) * lax.rsqrt(spread + 1e-06) * (1.0 + scale) + shift).astype(jnp.bfloat16)

def reference(tokens, slots, counts, shift, scale, gate, w_qkv, w_out):
    nblk = TOKENS // BLK
    onehot = (slots.reshape(nblk, BLK)[:, :, None] == jnp.arange(BLK, dtype=jnp.int32)[None, None, :]).astype(jnp.float32)
    sums = jnp.einsum('bts,btd->bsd', onehot, tokens.reshape(nblk, BLK, D).astype(jnp.float32))
    members = lax.optimization_barrier(jnp.sum(onehot, axis=1))
    merged = (sums / jnp.maximum(members, 1.0)[:, :, None]).astype(jnp.bfloat16).reshape(TOKENS, D)
    normed = layer_norm(merged, shift, scale)
    qkv = jnp.dot(normed, w_qkv, preferred_element_type=jnp.float32)
    query = qkv[:, :D].astype(jnp.bfloat16).reshape(TOKENS, HEADS, HD).transpose(1, 0, 2)
    keys = qkv[:, D:2 * D].astype(jnp.bfloat16).reshape(TOKENS, HEADS, HD).transpose(1, 0, 2)
    values = qkv[:, 2 * D:].astype(jnp.bfloat16).reshape(TOKENS, HEADS, HD).transpose(1, 0, 2)
    live = (jnp.arange(BLK, dtype=jnp.int32)[None, :] < counts[:, None]).reshape(TOKENS)
    bias = jnp.where(live, jnp.log(jnp.maximum(members.reshape(TOKENS), 1.0)), -1e+30).astype(jnp.float32)
    inverse = 1.0 / HD ** 0.5

    def one_head(items):
        qh, kh, vh = items
        score = jnp.dot(qh, kh.T, preferred_element_type=jnp.float32) * inverse + bias[None, :]
        top = lax.optimization_barrier(jnp.max(score, axis=-1, keepdims=True))
        probs = jnp.exp(score - top)
        total = lax.optimization_barrier(jnp.sum(probs, axis=-1, keepdims=True))
        return jnp.dot(probs.astype(jnp.bfloat16), vh, preferred_element_type=jnp.float32) / total
    heads_out = lax.map(one_head, (query, keys, values))
    attended = heads_out.transpose(1, 0, 2).reshape(TOKENS, D).astype(jnp.bfloat16)
    projected = jnp.dot(attended, w_out, preferred_element_type=jnp.float32)
    branch = jnp.einsum('bts,bsd->btd', onehot, projected.reshape(nblk, BLK, D), precision=lax.Precision.HIGHEST).reshape(TOKENS, D)
    return (tokens.astype(jnp.float32) + gate * branch).astype(jnp.bfloat16)
```

```python
import functools
import math

import jax
import jax.numpy as jnp
from jax import lax
from jax.experimental import pallas as pl
from jax.experimental.pallas import tpu as pltpu
from jax.sharding import PartitionSpec as P

HEADS = 16
BLK = 128
AUG = 8
CHUNK = 384
MESH = pl.DeviceIdType.MESH


def layer_norm(merged, shift, scale):
    values = merged.astype(jnp.float32)
    center = jnp.mean(values, axis=-1, keepdims=True)
    spread = jnp.mean((values - center) ** 2, axis=-1, keepdims=True)
    return ((values - center) * lax.rsqrt(spread + 1e-06) * (1.0 + scale) + shift).astype(
        jnp.bfloat16
    )


def merge(tokens, slots, counts):
    rows, width = tokens.shape
    nblk = rows // BLK
    onehot = slots.reshape(nblk, BLK)[:, :, None] == jnp.arange(BLK, dtype=jnp.int32)[None, None, :]
    sums = jnp.einsum(
        "bts,btd->bsd",
        onehot.astype(jnp.bfloat16),
        tokens.reshape(nblk, BLK, width),
        preferred_element_type=jnp.float32,
    )
    members = jnp.sum(onehot.astype(jnp.float32), axis=1)
    merged = (
        (sums / jnp.maximum(members, 1.0)[:, :, None]).astype(jnp.bfloat16).reshape(rows, width)
    )
    alive = (jnp.arange(BLK, dtype=jnp.int32)[None, :] < counts[:, None]).reshape(rows)
    bias = jnp.where(alive, jnp.log(jnp.maximum(members, 1.0)).reshape(rows), -1e30)
    return onehot, merged, bias


def flip(a, mask):
    out, bit = a, 1
    while bit <= mask:
        if mask & bit:
            out = out + bit * (1 - 2 * lax.rem(lax.div(a, bit), 2))
        bit *= 2
    return out


def attention(
    n, hd, slots, counts, tokens, shift, scale, w_hbm, out, w, turned, kv_msg, q_msg,
    kv_in, q_in, qs, ks, vs, scores, part, w_sem, *sems
):
    kv_out_sem, kv_in_sem, q_out_sem, q_in_sem, r_out_sem, r_in_sem = sems
    me = lax.axis_index("patch")
    rows, width = tokens.shape
    aug = hd + AUG
    factor = math.log2(math.e) / math.sqrt(hd)

    def weights(p):
        return pltpu.make_async_copy(w_hbm.at[:, pl.ds(p * width, width)], w.at[p], w_sem.at[p])

    for p in (1, 2, 0):
        weights(p).start()
    barrier = pltpu.get_barrier_semaphore()
    for i in range(1, n):
        pl.semaphore_signal(
            barrier, inc=1, device_id={"patch": lax.rem(me + i, n)}, device_id_type=MESH
        )

    slot = lax.broadcasted_iota(jnp.int32, (rows, rows), 0)
    exact = (slots[...] == jnp.where(slot < counts[...], slot, 0)).astype(jnp.float32)
    picks = exact.astype(jnp.bfloat16)
    sums = jnp.dot(picks, tokens[...], preferred_element_type=jnp.float32)
    members = jnp.sum(exact, axis=1, keepdims=True)
    merged = (sums / jnp.maximum(members, 1.0)).astype(jnp.bfloat16)
    normed = layer_norm(merged, shift[...][None], scale[...][None])
    sizes = lax.dot_general(
        jnp.ones((AUG, rows), jnp.bfloat16),
        picks,
        (((1,), (1,)), ((), ())),
        preferred_element_type=jnp.float32,
    )
    alive = lax.broadcasted_iota(jnp.int32, (AUG, rows), 1) < counts[...]
    sizes = jnp.where(alive, sizes, 0.0)

    def project(p):
        weights(p).wait()
        for at in range(0, width, CHUNK):
            piece = jnp.dot(normed, w[p, :, at : at + CHUNK], preferred_element_type=jnp.float32)
            turned[at : at + CHUNK] = piece.T

    def head(h):
        return turned[h * hd : (h + 1) * hd]

    project(1)
    for h in range(n):
        kv_msg[h, :hd] = head(h).astype(jnp.bfloat16)
    project(2)
    for h in range(n):
        kv_msg[h, hd:] = jnp.concatenate([head(h) * sizes[:1], sizes], axis=0).astype(jnp.bfloat16)

    def copy(src_ref, dst_ref, send, recv, dst, src):
        return pltpu.make_async_remote_copy(
            src_ref=src_ref.at[dst],
            dst_ref=dst_ref.at[src],
            send_sem=send.at[dst],
            recv_sem=recv.at[src],
            device_id={"patch": dst},
            device_id_type=MESH,
        )

    def kv_to(dst, src):
        return copy(kv_msg, kv_in, kv_out_sem, kv_in_sem, dst, src)

    def q_to(dst, src):
        return copy(q_msg, q_in, q_out_sem, q_in_sem, dst, src)

    def result_to(dst, src):
        return copy(part, out, r_out_sem, r_in_sem, dst, src)

    pl.semaphore_wait(barrier, n - 1)
    for i in range(n - 1, 0, -1):
        kv_to(flip(me, i), me).start()
    project(0)
    for h in range(n):
        q_msg[h] = (head(h) * factor).astype(jnp.bfloat16)
    for i in range(n - 1, 0, -1):
        q_to(flip(me, i), me).start()

    def span(index, size):
        return pl.ds(pl.multiple_of(index * size, size), size)

    def place_kv(src, block):
        ks[span(src, rows)] = block[:hd].astype(jnp.float32).T.astype(jnp.bfloat16)
        vs[:, span(src, rows)] = block[hd:]

    place_kv(me, kv_msg[me])
    for i in range(1, n):
        src = flip(me, i)
        kv_to(src, src).wait_recv()
        place_kv(src, kv_in[src])

    wide = 2 * rows
    pairs = n // 2
    total = n * rows
    mine = lax.div(me, 2)

    def pair_of(c):
        return flip(mine, c)

    def gather_queries(c):
        for t in range(2):
            src = 2 * pair_of(c) + t

            @pl.when(src != me)
            def _():
                q_to(src, src).wait_recv()
                qs[c % 2, :, t * rows : (t + 1) * rows] = q_in[src]

            @pl.when(src == me)
            def _():
                qs[c % 2, :, t * rows : (t + 1) * rows] = q_msg[me]

    def step(c, top):
        peak = jnp.full((8, wide), -jnp.inf, jnp.float32)
        acc = jnp.zeros((aug, wide), jnp.float32)
        for at in range(0, total, wide):
            if c + 1 < pairs:
                score = jnp.dot(
                    ks[at : at + wide], qs[(c + 1) % 2], preferred_element_type=jnp.float32
                )
                scores[(c + 1) % 2, at : at + wide] = score
                peak = jnp.maximum(peak, jnp.max(score.reshape(wide // 8, 8, wide), axis=0))
            if c >= 0:
                probs = jnp.exp2(scores[c % 2, at : at + wide] - top).astype(jnp.bfloat16)
                acc += jnp.dot(vs[:, at : at + wide], probs, preferred_element_type=jnp.float32)
        if c >= 0:
            done = (acc[:hd] / acc[hd : hd + 1]).astype(jnp.bfloat16)
            for t in range(2):
                dst = 2 * pair_of(c) + t
                part[dst] = done[:, t * rows : (t + 1) * rows]

                @pl.when(dst != me)
                def _():
                    result_to(dst, me).start()

                @pl.when(dst == me)
                def _():
                    out[me] = part[me]

        return jnp.max(peak, axis=0, keepdims=True)

    top = None
    for c in range(-1, pairs):
        if c + 1 < pairs:
            gather_queries(c + 1)
        top = step(c, top)

    for i in range(1, n):
        other = flip(me, i)
        kv_to(other, me).wait_send()
        q_to(other, me).wait_send()
        result_to(other, me).wait_send()
        result_to(other, other).wait_recv()


def heads_apart(n, width, tokens, slots, counts, shift, scale, gate, w_qkv, w_out):
    rows = tokens.shape[0]
    hd = width // HEADS
    aug = hd + AUG
    vmem = pl.BlockSpec(memory_space=pltpu.VMEM)
    attended = pl.pallas_call(
        functools.partial(attention, n, hd),
        out_shape=jax.ShapeDtypeStruct((n, hd, rows), jnp.bfloat16),
        in_specs=[vmem] * 5 + [pl.BlockSpec(memory_space=pl.ANY)],
        out_specs=vmem,
        scratch_shapes=[
            pltpu.VMEM((3, width, width), jnp.bfloat16),
            pltpu.VMEM((width, rows), jnp.float32),
            pltpu.VMEM((n, hd + aug, rows), jnp.bfloat16),
            pltpu.VMEM((n, hd, rows), jnp.bfloat16),
            pltpu.VMEM((n, hd + aug, rows), jnp.bfloat16),
            pltpu.VMEM((n, hd, rows), jnp.bfloat16),
            pltpu.VMEM((2, hd, 2 * rows), jnp.bfloat16),
            pltpu.VMEM((n * rows, hd), jnp.bfloat16),
            pltpu.VMEM((aug, n * rows), jnp.bfloat16),
            pltpu.VMEM((2, n * rows, 2 * rows), jnp.float32),
            pltpu.VMEM((n, hd, rows), jnp.bfloat16),
            pltpu.SemaphoreType.DMA((3,)),
        ]
        + [pltpu.SemaphoreType.DMA((n,))] * 6,
        compiler_params=pltpu.CompilerParams(
            collective_id=0, has_side_effects=True, vmem_limit_bytes=56 * 1024 * 1024
        ),
    )(slots[None], counts[None], tokens, shift, scale, w_qkv)
    attended = attended.reshape(width, rows)
    onehot = slots[:, None] == jnp.arange(rows, dtype=jnp.int32)[None, :]
    picked = lax.dot_general(
        onehot.astype(jnp.bfloat16),
        attended,
        (((1,), (1,)), ((), ())),
        preferred_element_type=jnp.float32,
    ).astype(jnp.bfloat16)
    branch = jnp.dot(picked, w_out, preferred_element_type=jnp.float32)
    return (tokens.astype(jnp.float32) + gate * branch).astype(jnp.bfloat16)


def rows_gathered(tokens, slots, counts, shift, scale, gate, w_qkv, w_out):
    rows, width = tokens.shape
    nblk = rows // BLK
    hd = width // HEADS
    onehot, merged, bias = merge(tokens, slots, counts)
    normed = layer_norm(merged, shift, scale)
    qkv = jnp.dot(normed, w_qkv, preferred_element_type=jnp.float32)
    query, keys, values = (
        qkv[:, i * width : (i + 1) * width].astype(jnp.bfloat16) for i in range(3)
    )
    keys = lax.all_gather(keys, "patch", axis=0, tiled=True).reshape(-1, HEADS, hd)
    values = lax.all_gather(values, "patch", axis=0, tiled=True).reshape(-1, HEADS, hd)
    bias = lax.all_gather(bias, "patch", axis=0, tiled=True)
    query = query.reshape(rows, HEADS, hd)
    score = jnp.einsum("qhe,khe->hqk", query, keys, preferred_element_type=jnp.float32)
    score = score / hd**0.5 + bias[None, None, :]
    probs = jnp.exp(score - jnp.max(score, axis=-1, keepdims=True))
    total = jnp.sum(probs, axis=-1)
    update = jnp.einsum(
        "hqk,khe->hqe", probs.astype(jnp.bfloat16), values, preferred_element_type=jnp.float32
    )
    attended = (update / total[:, :, None]).transpose(1, 0, 2).reshape(rows, width)
    picked = jnp.einsum(
        "bts,bsd->btd",
        onehot.astype(jnp.bfloat16),
        attended.astype(jnp.bfloat16).reshape(nblk, BLK, width),
        preferred_element_type=jnp.float32,
    ).astype(jnp.bfloat16)
    branch = jnp.dot(picked.reshape(rows, width), w_out, preferred_element_type=jnp.float32)
    return (tokens.astype(jnp.float32) + gate * branch).astype(jnp.bfloat16)


def solution(mesh):
    n = mesh.shape["patch"]

    def body(tokens, *rest):
        if n == HEADS and tokens.shape[0] == BLK:
            return heads_apart(n, tokens.shape[1], tokens, *rest)
        return rows_gathered(tokens, *rest)

    return jax.shard_map(
        body,
        mesh=mesh,
        in_specs=(
            P(("batch", "patch"), None),
            P(("batch", "patch")),
            P(("batch", "patch")),
            P(),
            P(),
            P(),
            P(),
            P(),
        ),
        out_specs=P(("batch", "patch"), None),
        check_vma=False,
    )
```

```python
import functools
import math

import jax
import jax.numpy as jnp
from jax import lax
from jax.experimental import pallas as pl
from jax.experimental.pallas import tpu as pltpu
from jax.sharding import PartitionSpec as P

HEADS = 16
BLK = 128
AUG = 8
CHUNK = 384
MESH = pl.DeviceIdType.MESH


def layer_norm(merged, shift, scale):
    values = merged.astype(jnp.float32)
    center = jnp.mean(values, axis=-1, keepdims=True)
    spread = jnp.mean((values - center) ** 2, axis=-1, keepdims=True)
    return ((values - center) * lax.rsqrt(spread + 1e-06) * (1.0 + scale) + shift).astype(
        jnp.bfloat16
    )


def merge(tokens, slots, counts):
    rows, width = tokens.shape
    nblk = rows // BLK
    onehot = slots.reshape(nblk, BLK)[:, :, None] == jnp.arange(BLK, dtype=jnp.int32)[None, None, :]
    sums = jnp.einsum(
        "bts,btd->bsd",
        onehot.astype(jnp.bfloat16),
        tokens.reshape(nblk, BLK, width),
        preferred_element_type=jnp.float32,
    )
    members = jnp.sum(onehot.astype(jnp.float32), axis=1)
    merged = (
        (sums / jnp.maximum(members, 1.0)[:, :, None]).astype(jnp.bfloat16).reshape(rows, width)
    )
    alive = (jnp.arange(BLK, dtype=jnp.int32)[None, :] < counts[:, None]).reshape(rows)
    bias = jnp.where(alive, jnp.log(jnp.maximum(members, 1.0)).reshape(rows), -1e30)
    return onehot, merged, bias


def flip(a, mask):
    out, bit = a, 1
    while bit <= mask:
        if mask & bit:
            out = out + bit * (1 - 2 * lax.rem(lax.div(a, bit), 2))
        bit *= 2
    return out


def attention(
    n, hd, slots_hbm, tokens_hbm, shift_hbm, scale_hbm, gate_hbm, w_hbm, wo_hbm, out, slots,
    tokens, shift, scale, gate, wo, back, r_in, w_far, w_near, turned, kv_msg, q_msg, kv_in, q_in, qs, ks, vs, scores, part,
    small_sem, w_sem, wo_sem, *sems
):
    kv_out_sem, kv_in_sem, q_out_sem, q_in_sem, r_out_sem, r_in_sem = sems
    me = lax.axis_index("patch")
    rows, width = tokens_hbm.shape
    aug = hd + AUG
    factor = math.log2(math.e) / math.sqrt(hd)

    half = n // 2
    cols = half * hd
    near_cols = -(-cols // 128) * 128
    far_cols = width - near_cols
    side = lax.div(me, half)
    near_at = pl.multiple_of(side * far_cols, 128)
    far_at = pl.multiple_of((1 - side) * near_cols, 128)

    def weights(p, far):
        at, size, dst = (far_at, far_cols, w_far) if far else (near_at, near_cols, w_near)
        start = pl.multiple_of(p * width + at, 128)
        return pltpu.make_async_copy(
            w_hbm.at[:, pl.ds(start, size)], dst.at[p], w_sem.at[2 * p + far]
        )

    barrier = pltpu.get_barrier_semaphore()
    for i in range(n - 1, 0, -1):
        pl.semaphore_signal(
            barrier, inc=1, device_id={"patch": flip(me, i)}, device_id_type=MESH
        )
    small = [
        pltpu.make_async_copy(src, dst, small_sem.at[i])
        for i, (src, dst) in enumerate(
            (
                (slots_hbm, slots),
                (tokens_hbm, tokens),
                (shift_hbm, shift),
                (scale_hbm, scale),
                (gate_hbm, gate),
            )
        )
    ]
    for item in small:
        item.start()
    for far in (0, 1):
        for p in (1, 2):
            weights(p, far).start()
    for far in (0, 1):
        weights(0, far).start()
    load_wo = pltpu.make_async_copy(wo_hbm, wo, wo_sem)
    load_wo.start()
    for item in small:
        item.wait()

    slot = lax.broadcasted_iota(jnp.int32, (rows, rows), 0)
    live = jnp.max(slots[...][None], axis=1, keepdims=True) + 1
    exact = (slots[...][None] == jnp.where(slot < live, slot, 0)).astype(jnp.float32)
    picks = exact.astype(jnp.bfloat16)
    back[...] = (slots[...][None] == slot).astype(jnp.float32).T.astype(jnp.bfloat16)
    sums = jnp.dot(picks, tokens[...], preferred_element_type=jnp.float32)
    members = jnp.sum(exact, axis=1, keepdims=True)
    merged = (sums / jnp.maximum(members, 1.0)).astype(jnp.bfloat16)
    normed = layer_norm(merged, shift[...][None], scale[...][None])
    sizes = lax.dot_general(
        jnp.ones((AUG, rows), jnp.bfloat16),
        picks,
        (((1,), (1,)), ((), ())),
        preferred_element_type=jnp.float32,
    )
    alive = lax.broadcasted_iota(jnp.int32, (AUG, rows), 1) < live
    sizes = jnp.where(alive, sizes, 0.0)

    def project(p, far):
        weights(p, far).wait()
        at, size, src = (far_at, far_cols, w_far) if far else (near_at, near_cols, w_near)
        piece = jnp.dot(normed, src[p], preferred_element_type=jnp.float32)
        turned[pl.ds(p * width + at, size)] = piece.T

    def heads(far):
        base = ((1 - side) if far else side) * half
        return [base + j for j in range(half)]

    def head(p, h):
        return turned[pl.ds(pl.multiple_of(p * width + h * hd, 8), hd)]

    def pack_kv(far):
        for h in heads(far):
            kv_msg[h, :hd] = head(1, h).astype(jnp.bfloat16)
            kv_msg[h, hd:] = jnp.concatenate([head(2, h) * sizes[:1], sizes], axis=0).astype(
                jnp.bfloat16
            )

    def pack_q(far):
        for h in heads(far):
            q_msg[h] = (head(0, h) * factor).astype(jnp.bfloat16)

    project(1, 0)
    project(2, 0)
    pack_kv(0)

    def copy(src_ref, dst_ref, send, recv, dst, src):
        return pltpu.make_async_remote_copy(
            src_ref=src_ref.at[dst],
            dst_ref=dst_ref.at[src],
            send_sem=send.at[dst],
            recv_sem=recv.at[src],
            device_id={"patch": dst},
            device_id_type=MESH,
        )

    def kv_to(dst, src):
        return copy(kv_msg, kv_in, kv_out_sem, kv_in_sem, dst, src)

    def q_to(dst, src):
        return copy(q_msg, q_in, q_out_sem, q_in_sem, dst, src)

    def result_to(dst, src):
        return copy(part, r_in, r_out_sem, r_in_sem, dst, src)

    pl.semaphore_wait(barrier, n - 1)
    for i in range(1, half):
        kv_to(flip(me, i), me).start()
    project(1, 1)
    project(2, 1)
    pack_kv(1)
    for i in range(half, n):
        kv_to(flip(me, i), me).start()
    project(0, 0)
    pack_q(0)
    for i in range(1, half):
        q_to(flip(me, i), me).start()
    project(0, 1)
    pack_q(1)
    for i in range(half, n):
        q_to(flip(me, i), me).start()
    def span(index, size):
        return pl.ds(pl.multiple_of(index * size, size), size)

    def place_kv(src, block):
        ks[span(src, rows)] = block[:hd].astype(jnp.float32).T.astype(jnp.bfloat16)
        vs[:, span(src, rows)] = block[hd:]

    place_kv(me, kv_msg[me])
    for i in range(1, n):
        src = flip(me, i)
        kv_to(src, src).wait_recv()
        place_kv(src, kv_in[src])

    wide = 2 * rows
    pairs = n // 2
    total = n * rows
    mine = lax.div(me, 2)

    def pair_of(c):
        return flip(mine, c)

    def gather_queries(c):
        for t in range(2):
            src = 2 * pair_of(c) + t

            @pl.when(src != me)
            def _():
                q_to(src, src).wait_recv()
                qs[c % 2, :, t * rows : (t + 1) * rows] = q_in[src]

            @pl.when(src == me)
            def _():
                qs[c % 2, :, t * rows : (t + 1) * rows] = q_msg[me]

    def step(c, top):
        peak = jnp.full((8, wide), -jnp.inf, jnp.float32)
        acc = jnp.zeros((aug, wide), jnp.float32)
        for at in range(0, total, wide):
            if c + 1 < pairs:
                score = jnp.dot(
                    ks[at : at + wide], qs[(c + 1) % 2], preferred_element_type=jnp.float32
                )
                scores[(c + 1) % 2, at : at + wide] = score
                peak = jnp.maximum(peak, jnp.max(score.reshape(wide // 8, 8, wide), axis=0))
            if c >= 0:
                probs = jnp.exp2(scores[c % 2, at : at + wide] - top).astype(jnp.bfloat16)
                acc += jnp.dot(vs[:, at : at + wide], probs, preferred_element_type=jnp.float32)
        if c >= 0:
            done = (acc[:hd] / acc[hd : hd + 1]).astype(jnp.bfloat16)
            for t in range(2):
                dst = 2 * pair_of(c) + t
                part[dst] = done[:, t * rows : (t + 1) * rows]

                @pl.when(dst != me)
                def _():
                    result_to(dst, me).start()

                @pl.when(dst == me)
                def _():
                    r_in[me] = part[me]

        return jnp.max(peak, axis=0, keepdims=True)

    top = None
    for c in range(-1, pairs):
        if c + 1 < pairs:
            gather_queries(c + 1)
        top = step(c, top)

    load_wo.wait()
    branch = jnp.zeros((rows, width), jnp.float32)
    deep = 2 * hd
    for c in range(pairs):
        pair = pair_of(c)
        for t in range(2):
            src = flip(me, 2 * c + t)
            if 2 * c + t:
                result_to(src, src).wait_recv()
        heads_in = jnp.concatenate([r_in[2 * pair], r_in[2 * pair + 1]], axis=0)
        picked = lax.dot_general(
            back[...], heads_in, (((1,), (1,)), ((), ())), preferred_element_type=jnp.float32
        ).astype(jnp.bfloat16)
        branch += jnp.dot(picked, wo[span(pair, deep)], preferred_element_type=jnp.float32)
    out[...] = (tokens[...].astype(jnp.float32) + gate[...][None] * branch).astype(jnp.bfloat16)

    for i in range(1, n):
        other = flip(me, i)
        kv_to(other, me).wait_send()
        q_to(other, me).wait_send()
        result_to(other, me).wait_send()


def heads_apart(n, width, tokens, slots, counts, shift, scale, gate, w_qkv, w_out):
    rows = tokens.shape[0]
    hd = width // HEADS
    aug = hd + AUG
    far_cols = width - -(-(n // 2 * hd) // 128) * 128
    vmem = pl.BlockSpec(memory_space=pltpu.VMEM)
    return pl.pallas_call(
        functools.partial(attention, n, hd),
        out_shape=pltpu.VMEM((rows, width), jnp.bfloat16),
        in_specs=[pl.BlockSpec(memory_space=pltpu.HBM)] * 7,
        out_specs=vmem,
        scratch_shapes=[
            pltpu.VMEM((rows,), jnp.int32),
            pltpu.VMEM((rows, width), jnp.bfloat16),
            pltpu.VMEM((width,), jnp.float32),
            pltpu.VMEM((width,), jnp.float32),
            pltpu.VMEM((width,), jnp.float32),
            pltpu.VMEM((width, width), jnp.bfloat16),
            pltpu.VMEM((rows, rows), jnp.bfloat16),
            pltpu.VMEM((n, hd, rows), jnp.bfloat16),
            pltpu.VMEM((3, width, far_cols), jnp.bfloat16),
            pltpu.VMEM((3, width, width - far_cols), jnp.bfloat16),
            pltpu.VMEM((3 * width, rows), jnp.float32),
            pltpu.VMEM((n, hd + aug, rows), jnp.bfloat16),
            pltpu.VMEM((n, hd, rows), jnp.bfloat16),
            pltpu.VMEM((n, hd + aug, rows), jnp.bfloat16),
            pltpu.VMEM((n, hd, rows), jnp.bfloat16),
            pltpu.VMEM((2, hd, 2 * rows), jnp.bfloat16),
            pltpu.VMEM((n * rows, hd), jnp.bfloat16),
            pltpu.VMEM((aug, n * rows), jnp.bfloat16),
            pltpu.VMEM((2, n * rows, 2 * rows), jnp.float32),
            pltpu.VMEM((n, hd, rows), jnp.bfloat16),
            pltpu.SemaphoreType.DMA((5,)),
            pltpu.SemaphoreType.DMA((6,)),
            pltpu.SemaphoreType.DMA,
        ]
        + [pltpu.SemaphoreType.DMA((n,))] * 6,
        compiler_params=pltpu.CompilerParams(
            collective_id=0, has_side_effects=True, vmem_limit_bytes=57 * 1024 * 1024
        ),
    )(slots, tokens, shift, scale, gate, w_qkv, w_out)


def rows_gathered(tokens, slots, counts, shift, scale, gate, w_qkv, w_out):
    rows, width = tokens.shape
    nblk = rows // BLK
    hd = width // HEADS
    onehot, merged, bias = merge(tokens, slots, counts)
    normed = layer_norm(merged, shift, scale)
    qkv = jnp.dot(normed, w_qkv, preferred_element_type=jnp.float32)
    query, keys, values = (
        qkv[:, i * width : (i + 1) * width].astype(jnp.bfloat16) for i in range(3)
    )
    keys = lax.all_gather(keys, "patch", axis=0, tiled=True).reshape(-1, HEADS, hd)
    values = lax.all_gather(values, "patch", axis=0, tiled=True).reshape(-1, HEADS, hd)
    bias = lax.all_gather(bias, "patch", axis=0, tiled=True)
    query = query.reshape(rows, HEADS, hd)
    score = jnp.einsum("qhe,khe->hqk", query, keys, preferred_element_type=jnp.float32)
    score = score / hd**0.5 + bias[None, None, :]
    probs = jnp.exp(score - jnp.max(score, axis=-1, keepdims=True))
    total = jnp.sum(probs, axis=-1)
    update = jnp.einsum(
        "hqk,khe->hqe", probs.astype(jnp.bfloat16), values, preferred_element_type=jnp.float32
    )
    attended = (update / total[:, :, None]).transpose(1, 0, 2).reshape(rows, width)
    picked = jnp.einsum(
        "bts,bsd->btd",
        onehot.astype(jnp.bfloat16),
        attended.astype(jnp.bfloat16).reshape(nblk, BLK, width),
        preferred_element_type=jnp.float32,
    ).astype(jnp.bfloat16)
    branch = jnp.dot(picked.reshape(rows, width), w_out, preferred_element_type=jnp.float32)
    return (tokens.astype(jnp.float32) + gate * branch).astype(jnp.bfloat16)


def solution(mesh):
    n = mesh.shape["patch"]

    def body(tokens, *rest):
        if n == HEADS and tokens.shape[0] == BLK:
            return heads_apart(n, tokens.shape[1], tokens, *rest)
        return rows_gathered(tokens, *rest)

    return jax.shard_map(
        body,
        mesh=mesh,
        in_specs=(
            P(("batch", "patch"), None),
            P(("batch", "patch")),
            P(("batch", "patch")),
            P(),
            P(),
            P(),
            P(),
            P(),
        ),
        out_specs=P(("batch", "patch"), None),
        check_vma=False,
    )
```

```python
import functools
import math

import jax
import jax.numpy as jnp
from jax import lax
from jax.experimental import pallas as pl
from jax.experimental.pallas import tpu as pltpu
from jax.sharding import PartitionSpec as P

HEADS = 16
BLK = 128
AUG = 8
CHUNK = 384
MESH = pl.DeviceIdType.MESH


def layer_norm(merged, shift, scale):
    values = merged.astype(jnp.float32)
    center = jnp.mean(values, axis=-1, keepdims=True)
    spread = jnp.mean((values - center) ** 2, axis=-1, keepdims=True)
    return ((values - center) * lax.rsqrt(spread + 1e-06) * (1.0 + scale) + shift).astype(
        jnp.bfloat16
    )


def merge(tokens, slots, counts):
    rows, width = tokens.shape
    nblk = rows // BLK
    onehot = slots.reshape(nblk, BLK)[:, :, None] == jnp.arange(BLK, dtype=jnp.int32)[None, None, :]
    sums = jnp.einsum(
        "bts,btd->bsd",
        onehot.astype(jnp.bfloat16),
        tokens.reshape(nblk, BLK, width),
        preferred_element_type=jnp.float32,
    )
    members = jnp.sum(onehot.astype(jnp.float32), axis=1)
    merged = (
        (sums / jnp.maximum(members, 1.0)[:, :, None]).astype(jnp.bfloat16).reshape(rows, width)
    )
    alive = (jnp.arange(BLK, dtype=jnp.int32)[None, :] < counts[:, None]).reshape(rows)
    bias = jnp.where(alive, jnp.log(jnp.maximum(members, 1.0)).reshape(rows), -1e30)
    return onehot, merged, bias


def flip(a, mask):
    out, bit = a, 1
    while bit <= mask:
        if mask & bit:
            out = out + bit * (1 - 2 * lax.rem(lax.div(a, bit), 2))
        bit *= 2
    return out


def attention(
    n, hd, slots_hbm, tokens_hbm, shift_hbm, scale_hbm, gate_hbm, w_hbm, wo_hbm, out, slots,
    tokens, shift, scale, gate, wo, back, r_in, w_broad, w_slim, turned, k_msg, v_msg, q_msg, m_msg, k_in, v_in, q_in, m_in,
    qs, ks, vs, scores, part,
    small_sem, w_sem, wo_sem, *sems
):
    k_sems, v_sems, q_sems, m_sems, r_sems = (sems[i : i + 2] for i in range(0, 10, 2))
    me = lax.axis_index("patch")
    rows, width = tokens_hbm.shape
    aug = hd + AUG
    factor = math.log2(math.e) / math.sqrt(hd)

    half = n // 2
    cols = half * hd
    broad = -(-cols // 128) * 128
    slim = width - broad
    side = lax.div(me, half)

    def chunk(p, far):
        early = (0, 1, 1)[p] == far
        size, buf = (broad, w_broad) if early else (slim, w_slim)
        at = ((1 - side) if far else side) * (width - size)
        return pl.multiple_of(at, 128), size, buf.at[p]

    def weights(p, far):
        at, size, buf = chunk(p, far)
        start = pl.multiple_of(p * width + at, 128)
        return pltpu.make_async_copy(w_hbm.at[:, pl.ds(start, size)], buf, w_sem.at[2 * p + far])

    barrier = pltpu.get_barrier_semaphore()
    for i in range(n - 1, 0, -1):
        pl.semaphore_signal(
            barrier, inc=1, device_id={"patch": flip(me, i)}, device_id_type=MESH
        )
    small = [
        pltpu.make_async_copy(src, dst, small_sem.at[i])
        for i, (src, dst) in enumerate(
            (
                (slots_hbm, slots),
                (tokens_hbm, tokens),
                (shift_hbm, shift),
                (scale_hbm, scale),
                (gate_hbm, gate),
            )
        )
    ]
    for item in small:
        item.start()
    for p, far in ((1, 1), (1, 0), (2, 1), (2, 0), (0, 0), (0, 1)):
        weights(p, far).start()
    load_wo = pltpu.make_async_copy(wo_hbm, wo, wo_sem)
    load_wo.start()
    for item in small:
        item.wait()

    slot = lax.broadcasted_iota(jnp.int32, (rows, rows), 0)
    live = jnp.max(slots[...][None], axis=1, keepdims=True) + 1
    exact = (slots[...][None] == jnp.where(slot < live, slot, 0)).astype(jnp.float32)
    picks = exact.astype(jnp.bfloat16)
    back[...] = (slots[...][None] == slot).astype(jnp.float32).T.astype(jnp.bfloat16)
    sums = jnp.dot(picks, tokens[...], preferred_element_type=jnp.float32)
    members = jnp.sum(exact, axis=1, keepdims=True)
    merged = (sums / jnp.maximum(members, 1.0)).astype(jnp.bfloat16)
    normed = layer_norm(merged, shift[...][None], scale[...][None])
    sizes = lax.dot_general(
        jnp.ones((AUG, rows), jnp.bfloat16),
        picks,
        (((1,), (1,)), ((), ())),
        preferred_element_type=jnp.float32,
    )
    alive = lax.broadcasted_iota(jnp.int32, (AUG, rows), 1) < live
    sizes = jnp.where(alive, sizes, 0.0)
    m_msg[...] = sizes[:1]

    def project(p, far):
        weights(p, far).wait()
        at, size, buf = chunk(p, far)
        piece = jnp.dot(normed, buf[...], preferred_element_type=jnp.float32)
        turned[pl.ds(p * width + at, size)] = piece.T

    def heads(far):
        base = ((1 - side) if far else side) * half
        return [base + j for j in range(half)]

    def head(p, h):
        return turned[pl.ds(pl.multiple_of(p * width + h * hd, 8), hd)]

    def pack(p, far):
        project(p, far)
        for h in heads(far):
            if p == 0:
                q_msg[h] = (head(0, h) * factor).astype(jnp.bfloat16)
            elif p == 1:
                k_msg[h] = head(1, h).astype(jnp.bfloat16)
            else:
                v_msg[h] = (head(2, h) * sizes[:1]).astype(jnp.bfloat16)

    def copy(src_ref, dst_ref, sems, dst, src):
        return pltpu.make_async_remote_copy(
            src_ref=src_ref,
            dst_ref=dst_ref.at[src],
            send_sem=sems[0].at[dst],
            recv_sem=sems[1].at[src],
            device_id={"patch": dst},
            device_id_type=MESH,
        )

    def k_to(dst, src):
        return copy(k_msg.at[dst], k_in, k_sems, dst, src)

    def v_to(dst, src):
        return copy(v_msg.at[dst], v_in, v_sems, dst, src)

    def q_to(dst, src):
        return copy(q_msg.at[dst], q_in, q_sems, dst, src)

    def m_to(dst, src):
        return copy(m_msg, m_in, m_sems, dst, src)

    def result_to(dst, src):
        return copy(part.at[dst], r_in, r_sems, dst, src)

    def send(to, far):
        for i in range(half, n) if far else range(1, half):
            to(flip(me, i), me).start()

    pack(1, 1)
    pl.semaphore_wait(barrier, n - 1)
    send(k_to, 1)
    send(m_to, 1)
    pack(1, 0)
    send(k_to, 0)
    send(m_to, 0)
    pack(2, 1)
    send(v_to, 1)
    pack(2, 0)
    send(v_to, 0)
    pack(0, 0)
    send(q_to, 0)
    pack(0, 1)
    send(q_to, 1)

    def span(index, size):
        return pl.ds(pl.multiple_of(index * size, size), size)

    def place_k(src, block):
        ks[span(src, rows)] = block.astype(jnp.float32).T.astype(jnp.bfloat16)

    def place_v(src, block, size):
        vs[:hd, span(src, rows)] = block
        vs[hd:, span(src, rows)] = jnp.broadcast_to(size, (AUG, rows)).astype(jnp.bfloat16)

    place_k(me, k_msg[me])
    place_v(me, v_msg[me], m_msg[...])
    for i in range(1, n):
        src = flip(me, i)
        k_to(src, src).wait_recv()
        place_k(src, k_in[src])
    for i in range(1, n):
        src = flip(me, i)
        m_to(src, src).wait_recv()
        v_to(src, src).wait_recv()
        place_v(src, v_in[src], m_in[src])

    wide = 2 * rows
    pairs = n // 2
    total = n * rows
    mine = lax.div(me, 2)
    turn = [pairs // 2 * (c % 2) + c // 2 for c in range(pairs)]

    def pair_of(c):
        return flip(mine, turn[c])

    def gather_queries(c):
        for t in range(2):
            src = 2 * pair_of(c) + t

            @pl.when(src != me)
            def _():
                q_to(src, src).wait_recv()
                qs[c % 2, :, t * rows : (t + 1) * rows] = q_in[src]

            @pl.when(src == me)
            def _():
                qs[c % 2, :, t * rows : (t + 1) * rows] = q_msg[me]

    def step(c, top):
        peak = jnp.full((8, wide), -jnp.inf, jnp.float32)
        acc = jnp.zeros((aug, wide), jnp.float32)
        for at in range(0, total, wide):
            if c + 1 < pairs:
                score = jnp.dot(
                    ks[at : at + wide], qs[(c + 1) % 2], preferred_element_type=jnp.float32
                )
                scores[(c + 1) % 2, at : at + wide] = score
                peak = jnp.maximum(peak, jnp.max(score.reshape(wide // 8, 8, wide), axis=0))
            if c >= 0:
                probs = jnp.exp2(scores[c % 2, at : at + wide] - top).astype(jnp.bfloat16)
                acc += jnp.dot(vs[:, at : at + wide], probs, preferred_element_type=jnp.float32)
        if c >= 0:
            done = (acc[:hd] / acc[hd : hd + 1]).astype(jnp.bfloat16)
            for t in range(2):
                dst = 2 * pair_of(c) + t
                part[dst] = done[:, t * rows : (t + 1) * rows]

                @pl.when(dst != me)
                def _():
                    result_to(dst, me).start()

                @pl.when(dst == me)
                def _():
                    r_in[me] = part[me]

        return jnp.max(peak, axis=0, keepdims=True)

    top = None
    for c in range(-1, pairs):
        if c + 1 < pairs:
            gather_queries(c + 1)
        top = step(c, top)

    load_wo.wait()
    branch = jnp.zeros((rows, width), jnp.float32)
    deep = 2 * hd
    for c in range(pairs):
        pair = pair_of(c)
        for t in range(2):
            src = flip(me, 2 * turn[c] + t)
            if 2 * turn[c] + t:
                result_to(src, src).wait_recv()
        heads_in = jnp.concatenate([r_in[2 * pair], r_in[2 * pair + 1]], axis=0)
        picked = lax.dot_general(
            back[...], heads_in, (((1,), (1,)), ((), ())), preferred_element_type=jnp.float32
        ).astype(jnp.bfloat16)
        branch += jnp.dot(picked, wo[span(pair, deep)], preferred_element_type=jnp.float32)
    out[...] = (tokens[...].astype(jnp.float32) + gate[...][None] * branch).astype(jnp.bfloat16)

    for i in range(1, n):
        other = flip(me, i)
        k_to(other, me).wait_send()
        v_to(other, me).wait_send()
        m_to(other, me).wait_send()
        q_to(other, me).wait_send()
        result_to(other, me).wait_send()


def heads_apart(n, width, tokens, slots, counts, shift, scale, gate, w_qkv, w_out):
    rows = tokens.shape[0]
    hd = width // HEADS
    aug = hd + AUG
    broad = -(-(n // 2 * hd) // 128) * 128
    vmem = pl.BlockSpec(memory_space=pltpu.VMEM)
    return pl.pallas_call(
        functools.partial(attention, n, hd),
        out_shape=pltpu.VMEM((rows, width), jnp.bfloat16),
        in_specs=[pl.BlockSpec(memory_space=pltpu.HBM)] * 7,
        out_specs=vmem,
        scratch_shapes=[
            pltpu.VMEM((rows,), jnp.int32),
            pltpu.VMEM((rows, width), jnp.bfloat16),
            pltpu.VMEM((width,), jnp.float32),
            pltpu.VMEM((width,), jnp.float32),
            pltpu.VMEM((width,), jnp.float32),
            pltpu.VMEM((width, width), jnp.bfloat16),
            pltpu.VMEM((rows, rows), jnp.bfloat16),
            pltpu.VMEM((n, hd, rows), jnp.bfloat16),
            pltpu.VMEM((3, width, broad), jnp.bfloat16),
            pltpu.VMEM((3, width, width - broad), jnp.bfloat16),
            pltpu.VMEM((3 * width, rows), jnp.float32),
            pltpu.VMEM((n, hd, rows), jnp.bfloat16),
            pltpu.VMEM((n, hd, rows), jnp.bfloat16),
            pltpu.VMEM((n, hd, rows), jnp.bfloat16),
            pltpu.VMEM((1, rows), jnp.float32),
            pltpu.VMEM((n, hd, rows), jnp.bfloat16),
            pltpu.VMEM((n, hd, rows), jnp.bfloat16),
            pltpu.VMEM((n, hd, rows), jnp.bfloat16),
            pltpu.VMEM((n, 1, rows), jnp.float32),
            pltpu.VMEM((2, hd, 2 * rows), jnp.bfloat16),
            pltpu.VMEM((n * rows, hd), jnp.bfloat16),
            pltpu.VMEM((aug, n * rows), jnp.bfloat16),
            pltpu.VMEM((2, n * rows, 2 * rows), jnp.float32),
            pltpu.VMEM((n, hd, rows), jnp.bfloat16),
            pltpu.SemaphoreType.DMA((5,)),
            pltpu.SemaphoreType.DMA((6,)),
            pltpu.SemaphoreType.DMA,
        ]
        + [pltpu.SemaphoreType.DMA((n,))] * 10,
        compiler_params=pltpu.CompilerParams(
            collective_id=0, has_side_effects=True, vmem_limit_bytes=57 * 1024 * 1024
        ),
    )(slots, tokens, shift, scale, gate, w_qkv, w_out)


def rows_gathered(tokens, slots, counts, shift, scale, gate, w_qkv, w_out):
    rows, width = tokens.shape
    nblk = rows // BLK
    hd = width // HEADS
    onehot, merged, bias = merge(tokens, slots, counts)
    normed = layer_norm(merged, shift, scale)
    qkv = jnp.dot(normed, w_qkv, preferred_element_type=jnp.float32)
    query, keys, values = (
        qkv[:, i * width : (i + 1) * width].astype(jnp.bfloat16) for i in range(3)
    )
    keys = lax.all_gather(keys, "patch", axis=0, tiled=True).reshape(-1, HEADS, hd)
    values = lax.all_gather(values, "patch", axis=0, tiled=True).reshape(-1, HEADS, hd)
    bias = lax.all_gather(bias, "patch", axis=0, tiled=True)
    query = query.reshape(rows, HEADS, hd)
    score = jnp.einsum("qhe,khe->hqk", query, keys, preferred_element_type=jnp.float32)
    score = score / hd**0.5 + bias[None, None, :]
    probs = jnp.exp(score - jnp.max(score, axis=-1, keepdims=True))
    total = jnp.sum(probs, axis=-1)
    update = jnp.einsum(
        "hqk,khe->hqe", probs.astype(jnp.bfloat16), values, preferred_element_type=jnp.float32
    )
    attended = (update / total[:, :, None]).transpose(1, 0, 2).reshape(rows, width)
    picked = jnp.einsum(
        "bts,bsd->btd",
        onehot.astype(jnp.bfloat16),
        attended.astype(jnp.bfloat16).reshape(nblk, BLK, width),
        preferred_element_type=jnp.float32,
    ).astype(jnp.bfloat16)
    branch = jnp.dot(picked.reshape(rows, width), w_out, preferred_element_type=jnp.float32)
    return (tokens.astype(jnp.float32) + gate * branch).astype(jnp.bfloat16)


def solution(mesh):
    n = mesh.shape["patch"]

    def body(tokens, *rest):
        if n == HEADS and tokens.shape[0] == BLK:
            return heads_apart(n, tokens.shape[1], tokens, *rest)
        return rows_gathered(tokens, *rest)

    return jax.shard_map(
        body,
        mesh=mesh,
        in_specs=(
            P(("batch", "patch"), None),
            P(("batch", "patch")),
            P(("batch", "patch")),
            P(),
            P(),
            P(),
            P(),
            P(),
        ),
        out_specs=P(("batch", "patch"), None),
        check_vma=False,
    )
```
